32 devices in a mesh: groups: 2 (over x), sph: 16 (over z, y, core).
Axes of the slice: x: 2, y: 2, z: 4, core: 2. Of those that a mesh axis runs over, the one named last changes fastest.
Arguments:
- positions: float32 [512, 3], P('sph'), may hold values from -8 to 8
- wave_vectors: float32 [256, 3], replicated, may hold values from -5 to 5
- pattern: float32 [2, 448, 256], replicated, may hold values from -6 to 6
- dir_index: int32 [64], P('groups'), parts along dimension 0, may hold values from 0 to 255
- mie: float32 [2, 448, 512], P(None, None, 'sph'), may hold values from -0.9 to 0.9
- trans_table: bfloat16 [8, 2, 448, 448], replicated, may hold values from -0.1875 to 0.1875
- pair_route: int32 [1024, 1], P('sph'), may hold values from 0 to 15; in each aligned block of 64 rows (0 to 63, 64 to 127, ...) at most 8 rows name the same one
- pair_source: int32 [1024], P('sph'), may hold values from 0 to 15
- pair_target: int32 [1024], P('sph'), may hold values from 0 to 15
- pair_class: int32 [1024], P('sph'), may hold values from 0 to 7
Outputs:
- scattered: bfloat16 [896, 32768], P(None, ('groups', 'sph')), parts along dimension 1
- extinction: float32 [64], P('groups'), parts along dimension 0
The draws below stay inside these ranges and needn't reach their ends.
There are 2 independent parts, one for each index of `groups`. The reference program is written for one: setup_inputs(seed, part) draws one part's arguments, and reference() takes and returns one part's arrays. A program takes and returns all parts, laid end to end along the dimension named above; an argument that names none is the same for every part. Nothing has to cross between parts.
Inputs may be any that keep to these rules, and one draw needn't show every extreme that they name: `pair_route`: among the rows of one device no device is named by more than 8 pairs, and in every draw some device is named by exactly 8 of them.
All inputs are finite; a program needn't handle non-finite values.
Results may differ from the reference program's by a relative error of at most 0.0051.
Values may be sent and summed in bfloat16 or wider, within the bound.
No kernel may reach another device: no remote copies, remote signals or barrier semaphores. Data moves between devices by JAX's collectives and lax.ppermute only.
A program may use at most 192 MiB of HBM per device.

```python
import math
import jax
import jax.numpy as jnp
import numpy as np
from jax import lax

MODES = 448
DIRS = 32
DIRTAB = 256
CLASSES = 8
BLOCK = 2
BLK_DEV = 16
PAIRS_DEV = 64
CAP = 8
SPHERES = 512
PAIRS = 1024
N_SPH = 16


def place_ends(drawn, key, smallest, high):
    extent = drawn.shape
    index_at = [jax.random.randint(jax.random.fold_in(key, axis), (), 0, extent[axis]) for axis in range(len(extent))]
    drawn = drawn.at[tuple(index_at)].set(smallest)
    longest = extent.index(max(extent))
    index_at[longest] = (index_at[longest] + 1) % extent[longest]
    return drawn.at[tuple(index_at)].set(high)


def shard_levels(stream_key, shape, shards, smallest, top_value):
    factor_of = 1.0
    for axis_at, shards_of in shards:
        heights = jax.random.uniform(jax.random.fold_in(jax.random.fold_in(stream_key, 6), axis_at), (shards_of,), jnp.float32, smallest / len(shards), top_value / len(shards))
        factor_of = factor_of * jnp.repeat(jnp.exp(heights), shape[axis_at] // shards_of).reshape((-1,) + (1,) * (len(shape) - 1 - axis_at))
    return factor_of


def shared_out(own_key, own, number, rows, number_of, top, bound, lean):
    order = jax.random.permutation(own_key, number_of)
    crowded, common = load_shares(number_of, rows * top, bound, lean, True), load_shares(number_of, rows * top, bound, lean, False)
    places = jnp.arange(number_of)

    def named(tallies, offset_by):
        used = int((tallies > 0).sum())
        fixed = max(1, used // 4)
        shifted = fixed + (places - fixed + offset_by * (used - fixed)) % max(1, number_of - fixed)
        return jnp.zeros((number_of,), jnp.int32).at[order[jnp.where(places < fixed, places, shifted)]].set(jnp.asarray(tallies, jnp.int32))

    tallies = jnp.where(number % 4 == 0, named(crowded, number // 4), named(common, number - number // 4 - 1))
    mixed = jax.random.permutation(jax.random.fold_in(own, 3), number_of)
    giver, sink = mixed[0:number_of // 2 * 2:2], mixed[1:number_of // 2 * 2:2]
    slack = jnp.minimum(tallies[giver] - 1, bound - tallies[sink]) // 2
    slack = jnp.where((giver == order[0]) | (sink == order[0]) | (tallies[sink] == 0), 0, jnp.maximum(slack, 0))
    shifted = jax.random.randint(jax.random.fold_in(own, 4), (number_of // 2,), 0, 1 << 20) % (slack + 1)
    tallies = tallies.at[giver].add(-shifted).at[sink].add(shifted)
    items = jnp.searchsorted(jnp.cumsum(tallies), jnp.arange(rows * top), side="right").astype(jnp.int32)
    table = items.reshape(top, rows).T
    table = table[jax.random.permutation(jax.random.fold_in(own, 1), rows)]
    offset_by = jax.random.randint(jax.random.fold_in(own, 2), (rows, 1), 0, top)
    return jnp.take_along_axis(table, (jnp.arange(top)[None, :] + offset_by) % top, axis=1)


def load_shares(count, total, bound, skew, full):
    portions = [(1 << 20) // math.isqrt(rank ** skew) + 1 for rank in range(1, count + 1)]
    largest = bound if full else min(bound, max(-(-total // count), total * portions[0] // sum(portions)))
    least = 1 if total - largest >= count - 1 else 0
    given, rest = [largest] + [least] * (count - 1), total - largest - least * (count - 1)
    while rest > 0:
        candidates = [i for i in range(1, count) if given[i] < largest] or [i for i in range(1, count) if given[i] < bound]
        pool, budget = sum([portions[i] for i in candidates]), rest
        for i in candidates:
            addition = min(bound - given[i], max(1, budget * portions[i] // pool), rest)
            given[i] = given[i] + addition
            rest = rest - addition
    return np.array(given)


def gaussian(key, shape, scale, most, kind=jnp.bfloat16):
    return jnp.clip(scale * jax.random.normal(key, shape, jnp.float32), -most, most).astype(kind)


def setup_inputs(seed: int = 0, part: int = 0) -> dict:
    key_list = jax.random.split(jax.random.key(seed), 11)
    part_splits = jax.random.split(jax.random.fold_in(key_list[10], part), 11)
    positions = jnp.clip(jax.random.uniform(key_list[0], (SPHERES, 3), jnp.float32, -8.0, 8.0) * shard_levels(key_list[0], (SPHERES, 3), ((0, 16),), -0.4, 0.0), -8.0, 8.0)
    wave_vectors = gaussian(key_list[1], (DIRTAB, 3), 1.0, 5.0, jnp.float32)
    pattern = gaussian(key_list[2], (2, MODES, DIRTAB), 1.0, 6.0, jnp.float32)
    dir_index = place_ends(jax.random.randint(part_splits[3], (DIRS,), 0, DIRTAB), jax.random.fold_in(part_splits[3], 1), 0, DIRTAB - 1).astype(jnp.int32)
    mie = jnp.clip(jax.random.uniform(key_list[4], (2, MODES, SPHERES), jnp.float32, -0.9, 0.9) * shard_levels(key_list[4], (2, MODES, SPHERES), ((2, 16),), -0.4, 0.0), -0.9, 0.9)
    trans_table = gaussian(key_list[5], (CLASSES, 2, MODES, MODES), (2 * MODES) ** -0.5, 0.1875)
    pair_route_keys = jax.random.split(jax.random.fold_in(key_list[6], 1), PAIRS // PAIRS_DEV)
    pair_route_turns = jax.random.permutation(jax.random.fold_in(key_list[6], 3), PAIRS // PAIRS_DEV)
    pair_route = jax.vmap(lambda own, number: shared_out(jax.random.fold_in(key_list[6], 2), own, number, PAIRS_DEV, N_SPH, 1, CAP, 2))(pair_route_keys, pair_route_turns).reshape((PAIRS, 1))
    pair_source = place_ends(jax.random.randint(key_list[7], (PAIRS,), 0, BLK_DEV), jax.random.fold_in(key_list[7], 1), 0, BLK_DEV - 1).astype(jnp.int32)
    pair_target = place_ends(jax.random.randint(key_list[8], (PAIRS,), 0, BLK_DEV), jax.random.fold_in(key_list[8], 1), 0, BLK_DEV - 1).astype(jnp.int32)
    pair_class = place_ends(jax.random.randint(key_list[9], (PAIRS,), 0, CLASSES), jax.random.fold_in(key_list[9], 1), 0, CLASSES - 1).astype(jnp.int32)
    return dict(positions=positions, wave_vectors=wave_vectors, pattern=pattern, dir_index=dir_index, mie=mie, trans_table=trans_table, pair_route=pair_route, pair_source=pair_source, pair_target=pair_target, pair_class=pair_class)


def reference(positions, wave_vectors, pattern, dir_index, mie, trans_table, pair_route, pair_source, pair_target, pair_class):
    directions = wave_vectors[dir_index]
    phases = positions[:, 0:1] * directions[None, :, 0] + positions[:, 1:2] * directions[None, :, 1] + positions[:, 2:3] * directions[None, :, 2]
    cosine = jnp.cos(phases)
    sine_part = jnp.sin(phases)
    chosen = pattern[:, :, dir_index]
    inc_real = cosine[None] * chosen[0][:, None, :] - sine_part[None] * chosen[1][:, None, :]
    inc_imag = cosine[None] * chosen[1][:, None, :] + sine_part[None] * chosen[0][:, None, :]
    mie_real = mie[0][:, :, None]
    mie_imag = mie[1][:, :, None]
    scat_real = mie_real * inc_real - mie_imag * inc_imag
    scat_imag = mie_real * inc_imag + mie_imag * inc_real
    coeffs = jnp.concatenate([scat_real, scat_imag], 0).astype(jnp.bfloat16)
    columns = BLOCK * DIRS
    block_count = SPHERES // BLOCK
    block_data = coeffs.reshape(2 * MODES, block_count, columns).transpose(1, 0, 2)
    owner = jnp.arange(PAIRS, dtype=jnp.int32) // PAIRS_DEV
    source_global = (owner * BLK_DEV + pair_source).astype(jnp.int32)
    target_global = (pair_route[:, 0] * BLK_DEV + pair_target).astype(jnp.int32)
    group_shape = (PAIRS // 8, 8)

    def add_group(field_sum, group_items):
        sources, targets, classes = group_items
        tables = trans_table[classes].astype(jnp.float32)
        values = block_data[sources].astype(jnp.float32)
        data_real = values[:, :MODES]
        data_imag = values[:, MODES:]
        highest = lax.Precision.HIGHEST
        part_real = jnp.einsum('kij,kjc->kic', tables[:, 0], data_real, precision=highest) - jnp.einsum('kij,kjc->kic', tables[:, 1], data_imag, precision=highest)
        part_imag = jnp.einsum('kij,kjc->kic', tables[:, 1], data_real, precision=highest) + jnp.einsum('kij,kjc->kic', tables[:, 0], data_imag, precision=highest)
        contribution = jnp.concatenate([part_real, part_imag], 1).astype(jnp.bfloat16)
        contribution = lax.optimization_barrier(contribution).astype(jnp.float32)
        return field_sum.at[targets].add(contribution), None

    initial = jnp.zeros((block_count, 2 * MODES, columns), jnp.float32)
    summed, unused = lax.scan(add_group, initial, (source_global.reshape(group_shape), target_global.reshape(group_shape), pair_class.astype(jnp.int32).reshape(group_shape)))
    summed = summed.transpose(1, 0, 2).reshape(2 * MODES, SPHERES, DIRS)
    total_real = inc_real + summed[:MODES]
    total_imag = inc_imag + summed[MODES:]
    out_real = mie_real * total_real - mie_imag * total_imag
    out_imag = mie_real * total_imag + mie_imag * total_real
    scattered = jnp.concatenate([out_real, out_imag], 0).reshape(2 * MODES, SPHERES * DIRS).astype(jnp.bfloat16)
    extinction = jnp.sum(inc_real * out_real + inc_imag * out_imag, axis=(0, 1))
    return (scattered, extinction)
```

```python
import jax
import jax.numpy as jnp
from jax import lax
from jax.experimental import pallas as pl
from jax.experimental.pallas import tpu as pltpu
from jax.sharding import PartitionSpec as P

BLOCK = 2
LANES = 128

HIGHEST_PRECISION = lax.Precision.HIGHEST


def field_kernel(
    starts,
    sources,
    own,
    cos_ref,
    sin_ref,
    pat_ref,
    mie_ref,
    table_ref,
    out_ref,
    ext_ref,
    sum_real,
    sum_imag,
    in_real,
    in_imag,
    in_neg,
    acc_real,
    acc_imag,
):
    step = pl.program_id(0)
    steps = pl.num_programs(0)
    dirs, modes = pat_ref.shape[1], pat_ref.shape[2]
    cols = BLOCK * dirs
    blocks = in_real.shape[0] // cols

    def phase_of(block):
        sphere = block * BLOCK
        tile = sphere // LANES
        shift = (LANES - sphere % LANES) % LANES
        return pltpu.roll(cos_ref[tile], shift, 1), pltpu.roll(sin_ref[tile], shift, 1)

    def incident(cosine, sine, j):
        c = cosine[:, j : j + 1]
        s = sine[:, j : j + 1]
        pr, pi = pat_ref[0], pat_ref[1]
        return c * pr - s * pi, c * pi + s * pr

    def mie_rows(block, j):
        sphere = block * BLOCK + j
        return mie_ref[0, pl.ds(sphere, 1), :], mie_ref[1, pl.ds(sphere, 1), :]

    def add_pair(q, first):
        block = sources[q]
        cosine, sine = phase_of(block)
        for j in range(BLOCK):
            ir, ii = incident(cosine, sine, j)
            mr, mi = mie_rows(block, j)
            rows = pl.ds(j * dirs, dirs)
            xr = mr * ir - mi * ii
            xi = mr * ii + mi * ir
            if first:
                sum_real[rows, :] = xr
                sum_imag[rows, :] = xi
            else:
                sum_real[rows, :] += xr
                sum_imag[rows, :] += xi

    def build(t, carry):
        low = starts[step * blocks + t]
        high = starts[step * blocks + t + 1]
        rows = pl.ds(pl.multiple_of(t * cols, cols), cols)

        @pl.when(high == low)
        def _():
            zero = jnp.zeros((cols, modes), jnp.bfloat16)
            in_real[rows, :] = zero
            in_imag[rows, :] = zero
            in_neg[rows, :] = zero

        @pl.when(high > low)
        def _():
            add_pair(low, True)

            def more(q, c):
                add_pair(q, False)
                return c

            lax.fori_loop(low + 1, high, more, 0)
            in_real[rows, :] = sum_real[...].astype(jnp.bfloat16)
            rounded = sum_imag[...].astype(jnp.bfloat16)
            in_imag[rows, :] = rounded
            in_neg[rows, :] = -rounded

        return carry

    lax.fori_loop(0, blocks, build, 0)

    def dot(a, b):
        return lax.dot_general(
            a, b, (((1,), (1,)), ((), ())), preferred_element_type=jnp.float32
        )

    table_real = table_ref[0, 0]
    table_imag = table_ref[0, 1]
    add_real = dot(in_real[...], table_real) + dot(in_neg[...], table_imag)
    add_imag = dot(in_real[...], table_imag) + dot(in_imag[...], table_real)

    @pl.when(step == 0)
    def _():
        acc_real[...] = add_real
        acc_imag[...] = add_imag

    @pl.when(step > 0)
    def _():
        acc_real[...] += add_real
        acc_imag[...] += add_imag

    @pl.when(step == steps - 1)
    def _():
        ext_ref[...] = jnp.zeros(ext_ref.shape, jnp.float32)
        per_tile = LANES // cols

        for tile in range(blocks // per_tile):
            real_rows, imag_rows = [], []
            for b in range(per_tile):
                local = tile * per_tile + b
                block = own[0] * blocks + local
                cosine, sine = phase_of(block)
                for j in range(BLOCK):
                    ir, ii = incident(cosine, sine, j)
                    mr, mi = mie_rows(block, j)
                    rows = pl.ds(local * cols + j * dirs, dirs)
                    tr = ir + acc_real[rows, :]
                    ti = ii + acc_imag[rows, :]
                    outr = mr * tr - mi * ti
                    outi = mr * ti + mi * tr
                    ext_ref[...] += ir * outr + ii * outi
                    real_rows.append(outr)
                    imag_rows.append(outi)
            at = pl.ds(tile * LANES, LANES)
            out_ref[0:modes, at] = jnp.concatenate(real_rows, 0).T.astype(jnp.bfloat16)
            out_ref[modes:, at] = jnp.concatenate(imag_rows, 0).T.astype(jnp.bfloat16)


def shards(
    positions,
    wave_vectors,
    pattern,
    dir_index,
    mie,
    trans_table,
    pair_route,
    pair_source,
    pair_target,
    pair_class,
):
    modes = pattern.shape[1]
    spheres = positions.shape[0]
    dirs = dir_index.shape[0]
    table_rows = wave_vectors.shape[0]
    classes = trans_table.shape[0]
    cols = BLOCK * dirs
    blocks = spheres // BLOCK
    devices = lax.axis_size("sph")
    me = lax.axis_index("sph")
    pair_count = pair_source.shape[0]
    capacity = max(2, 2 * pair_count // devices)
    slots = devices * capacity
    all_spheres = devices * spheres
    all_pairs = devices * pair_count

    small = jnp.concatenate(
        [
            positions.T.reshape(-1),
            pair_route[:, 0].astype(jnp.float32),
            pair_source.astype(jnp.float32),
            (pair_class * blocks + pair_target).astype(jnp.float32),
        ]
    )
    small = lax.all_gather(small, "sph", axis=0)
    mie_rows = lax.all_gather(mie.transpose(0, 2, 1), "sph", axis=1, tiled=True)

    everywhere = small[:, : 3 * spheres].reshape(devices, 3, spheres)
    listed = small[:, 3 * spheres :].reshape(devices, 3, pair_count).astype(jnp.int32)
    route = listed[:, 0].reshape(-1)
    source = (listed[:, 1] + jnp.arange(devices, dtype=jnp.int32)[:, None] * blocks).reshape(-1)
    slot_key = listed[:, 2].reshape(-1)
    key_count = classes * blocks
    key = jnp.where(route == me, slot_key, key_count)
    starts = jnp.sum(
        (key[None, :] < jnp.arange(key_count + 1, dtype=jnp.int32)[:, None]).astype(jnp.int32), 1
    )
    unique = key * all_pairs + jnp.arange(all_pairs, dtype=jnp.int32)
    place = jnp.sum((unique[None, :] < unique[:, None]).astype(jnp.int32), 1)
    sources = jnp.sum(
        jnp.where(place[None, :] == jnp.arange(slots, dtype=jnp.int32)[:, None], source[None, :], 0),
        1,
    )

    select = (jnp.arange(table_rows, dtype=jnp.int32)[:, None] == dir_index[None, :]).astype(
        jnp.float32
    )
    directions = jnp.dot(select.T, wave_vectors, precision=HIGHEST_PRECISION)
    chosen = jnp.einsum("cmt,td->cdm", pattern, select, precision=HIGHEST_PRECISION)
    tiles = -(-all_spheres // LANES)
    place3 = everywhere.transpose(1, 0, 2).reshape(3, all_spheres)
    place3 = jnp.pad(place3, ((0, 0), (0, tiles * LANES - all_spheres))).reshape(
        3, tiles, 1, LANES
    )
    phases = (
        place3[0] * directions[None, :, 0:1]
        + place3[1] * directions[None, :, 1:2]
        + place3[2] * directions[None, :, 2:3]
    )
    cosine = jnp.cos(phases)
    sine = jnp.sin(phases)

    whole = lambda *shape: pl.BlockSpec(shape, lambda c, *_: (0,) * len(shape))
    scattered, terms = pl.pallas_call(
        field_kernel,
        grid_spec=pltpu.PrefetchScalarGridSpec(
            num_scalar_prefetch=3,
            grid=(classes,),
            in_specs=[
                whole(*cosine.shape),
                whole(*sine.shape),
                whole(2, dirs, modes),
                whole(2, all_spheres, modes),
                pl.BlockSpec((1, 2, modes, modes), lambda c, *_: (c, 0, 0, 0)),
            ],
            out_specs=[whole(2 * modes, spheres * dirs), whole(dirs, modes)],
            scratch_shapes=[
                pltpu.VMEM((cols, modes), jnp.float32),
                pltpu.VMEM((cols, modes), jnp.float32),
                pltpu.VMEM((blocks * cols, modes), jnp.bfloat16),
                pltpu.VMEM((blocks * cols, modes), jnp.bfloat16),
                pltpu.VMEM((blocks * cols, modes), jnp.bfloat16),
                pltpu.VMEM((blocks * cols, modes), jnp.float32),
                pltpu.VMEM((blocks * cols, modes), jnp.float32),
            ],
        ),
        out_shape=[
            jax.ShapeDtypeStruct((2 * modes, spheres * dirs), jnp.bfloat16),
            jax.ShapeDtypeStruct((dirs, modes), jnp.float32),
        ],
        compiler_params=pltpu.CompilerParams(
            dimension_semantics=("arbitrary",), vmem_limit_bytes=56 * 1024 * 1024
        ),
    )(
        starts,
        sources,
        jnp.full((1,), me, jnp.int32),
        cosine,
        sine,
        chosen,
        mie_rows,
        trans_table,
    )
    extinction = lax.psum(jnp.sum(terms, axis=1), "sph")
    return (scattered, extinction)


def solution(mesh):
    placed = (
        P("sph", None),
        P(),
        P(),
        P("groups"),
        P(None, None, "sph"),
        P(),
        P("sph", None),
        P("sph"),
        P("sph"),
        P("sph"),
    )
    return jax.shard_map(
        shards,
        mesh=mesh,
        in_specs=placed,
        out_specs=(P(None, ("groups", "sph")), P("groups")),
        check_vma=False,
    )
```

```python
import jax
import jax.numpy as jnp
from jax import lax
from jax.experimental import pallas as pl
from jax.experimental.pallas import tpu as pltpu
from jax.sharding import PartitionSpec as P

BLOCK = 2
LANES = 128

HIGHEST_PRECISION = lax.Precision.HIGHEST


def field_kernel(
    starts,
    sources,
    own,
    cos_ref,
    sin_ref,
    pat_ref,
    mie_ref,
    table_ref,
    out_ref,
    ext_ref,
    sum_real,
    sum_imag,
    in_real,
    in_imag,
    in_neg,
    acc_real,
    acc_imag,
):
    step = pl.program_id(0)
    steps = pl.num_programs(0)
    dirs, modes = pat_ref.shape[1], pat_ref.shape[2]
    cols = BLOCK * dirs
    blocks = in_real.shape[0] // cols

    def phase_of(block):
        sphere = block * BLOCK
        tile = sphere // LANES
        shift = (LANES - sphere % LANES) % LANES
        return pltpu.roll(cos_ref[tile], shift, 1), pltpu.roll(sin_ref[tile], shift, 1)

    def incident(cosine, sine, j):
        c = cosine[:, j : j + 1]
        s = sine[:, j : j + 1]
        pr, pi = pat_ref[0], pat_ref[1]
        return c * pr - s * pi, c * pi + s * pr

    def mie_rows(block, j):
        sphere = block * BLOCK + j
        return mie_ref[0, pl.ds(sphere, 1), :], mie_ref[1, pl.ds(sphere, 1), :]

    def add_pair(q, first):
        block = sources[q]
        cosine, sine = phase_of(block)
        for j in range(BLOCK):
            ir, ii = incident(cosine, sine, j)
            mr, mi = mie_rows(block, j)
            rows = pl.ds(j * dirs, dirs)
            xr = mr * ir - mi * ii
            xi = mr * ii + mi * ir
            if first:
                sum_real[rows, :] = xr
                sum_imag[rows, :] = xi
            else:
                sum_real[rows, :] += xr
                sum_imag[rows, :] += xi

    def build(t, carry):
        low = starts[step * blocks + t]
        high = starts[step * blocks + t + 1]
        rows = pl.ds(pl.multiple_of(t * cols, cols), cols)

        @pl.when(high == low)
        def _():
            zero = jnp.zeros((cols, modes), jnp.bfloat16)
            in_real[rows, :] = zero
            in_imag[rows, :] = zero
            in_neg[rows, :] = zero

        @pl.when(high > low)
        def _():
            add_pair(low, True)

            def more(q, c):
                add_pair(q, False)
                return c

            lax.fori_loop(low + 1, high, more, 0)
            in_real[rows, :] = sum_real[...].astype(jnp.bfloat16)
            rounded = sum_imag[...].astype(jnp.bfloat16)
            in_imag[rows, :] = rounded
            in_neg[rows, :] = -rounded

        return carry

    lax.fori_loop(0, blocks, build, 0)

    def dot(a, b):
        return lax.dot_general(
            a, b, (((1,), (1,)), ((), ())), preferred_element_type=jnp.float32
        )

    table_real = table_ref[0, 0]
    table_imag = table_ref[0, 1]
    add_real = dot(in_real[...], table_real) + dot(in_neg[...], table_imag)
    add_imag = dot(in_real[...], table_imag) + dot(in_imag[...], table_real)

    @pl.when(step == 0)
    def _():
        acc_real[...] = add_real
        acc_imag[...] = add_imag

    @pl.when(step > 0)
    def _():
        acc_real[...] += add_real
        acc_imag[...] += add_imag

    @pl.when(step == steps - 1)
    def _():
        ext_ref[...] = jnp.zeros(ext_ref.shape, jnp.float32)
        per_tile = LANES // cols

        for tile in range(blocks // per_tile):
            real_rows, imag_rows = [], []
            for b in range(per_tile):
                local = tile * per_tile + b
                block = own[0] * blocks + local
                cosine, sine = phase_of(block)
                for j in range(BLOCK):
                    ir, ii = incident(cosine, sine, j)
                    mr, mi = mie_rows(block, j)
                    rows = pl.ds(local * cols + j * dirs, dirs)
                    tr = ir + acc_real[rows, :]
                    ti = ii + acc_imag[rows, :]
                    outr = mr * tr - mi * ti
                    outi = mr * ti + mi * tr
                    ext_ref[...] += ir * outr + ii * outi
                    real_rows.append(outr)
                    imag_rows.append(outi)
            at = pl.ds(tile * LANES, LANES)
            out_ref[0:modes, at] = jnp.concatenate(real_rows, 0).T.astype(jnp.bfloat16)
            out_ref[modes:, at] = jnp.concatenate(imag_rows, 0).T.astype(jnp.bfloat16)


def exact_parts(x):
    first = lax.reduce_precision(x, 8, 7)
    second = lax.reduce_precision(x - first, 8, 7)
    third = (x - first) - second
    return jnp.stack([first, second, third])


def shards(
    positions,
    wave_vectors,
    pattern,
    dir_index,
    mie,
    trans_table,
    pair_route,
    pair_source,
    pair_target,
    pair_class,
):
    modes = pattern.shape[1]
    spheres = positions.shape[0]
    dirs = dir_index.shape[0]
    table_rows = wave_vectors.shape[0]
    classes = trans_table.shape[0]
    cols = BLOCK * dirs
    blocks = spheres // BLOCK
    devices = lax.axis_size("sph")
    me = lax.axis_index("sph")
    pair_count = pair_source.shape[0]
    capacity = max(2, 2 * pair_count // devices)
    slots = devices * capacity
    all_spheres = devices * spheres
    all_pairs = devices * pair_count

    own_mie = mie.transpose(0, 2, 1)
    rows = own_mie.astype(jnp.bfloat16).reshape(-1, LANES)
    cut = rows.shape[0]
    small = jnp.concatenate(
        [
            exact_parts(positions.T.reshape(-1)).reshape(-1),
            pair_route[:, 0].astype(jnp.float32),
            pair_source.astype(jnp.float32),
            pair_target.astype(jnp.float32),
            pair_class.astype(jnp.float32),
        ]
    )
    size = small.shape[0]
    small = jnp.pad(small, (0, -size % (16 * LANES))).reshape(-1, LANES)
    gathered = lax.all_gather(rows, "sph", axis=0)
    tail = lax.all_to_all(
        jnp.broadcast_to(small[None], (devices,) + small.shape), "sph", 0, 0, tiled=True
    ).reshape(devices, -1)
    mie_rows = gathered[:, :cut].reshape(devices, 2, spheres, modes).astype(jnp.float32)
    mie_rows = mie_rows.transpose(1, 0, 2, 3).reshape(2, all_spheres, modes)
    mie_rows = lax.dynamic_update_slice(mie_rows, own_mie, (0, me * spheres, 0))
    split = 9 * spheres
    pieces = tail[:, :split].reshape(devices, 3, 3, spheres)
    everywhere = (pieces[:, 2] + pieces[:, 1]) + pieces[:, 0]
    listed = tail[:, split:size].reshape(devices, 4, pair_count).astype(jnp.int32)
    route = listed[:, 0].reshape(-1)
    source = (listed[:, 1] + jnp.arange(devices, dtype=jnp.int32)[:, None] * blocks).reshape(-1)
    slot_key = (listed[:, 3] * blocks + listed[:, 2]).reshape(-1)
    key_count = classes * blocks
    key = jnp.where(route == me, slot_key, key_count)
    starts = jnp.sum(
        (key[None, :] < jnp.arange(key_count + 1, dtype=jnp.int32)[:, None]).astype(jnp.int32), 1
    )
    unique = key * all_pairs + jnp.arange(all_pairs, dtype=jnp.int32)
    place = jnp.sum((unique[None, :] < unique[:, None]).astype(jnp.int32), 1)
    sources = jnp.sum(
        jnp.where(place[None, :] == jnp.arange(slots, dtype=jnp.int32)[:, None], source[None, :], 0),
        1,
    )

    select = (jnp.arange(table_rows, dtype=jnp.int32)[:, None] == dir_index[None, :]).astype(
        jnp.float32
    )
    directions = jnp.dot(select.T, wave_vectors, precision=HIGHEST_PRECISION)
    chosen = jnp.einsum("cmt,td->cdm", pattern, select, precision=HIGHEST_PRECISION)
    tiles = -(-all_spheres // LANES)
    place3 = everywhere.transpose(1, 0, 2).reshape(3, all_spheres)
    place3 = jnp.pad(place3, ((0, 0), (0, tiles * LANES - all_spheres))).reshape(
        3, tiles, 1, LANES
    )
    phases = (
        place3[0] * directions[None, :, 0:1]
        + place3[1] * directions[None, :, 1:2]
        + place3[2] * directions[None, :, 2:3]
    )
    cosine = jnp.cos(phases)
    sine = jnp.sin(phases)

    whole = lambda *shape: pl.BlockSpec(shape, lambda c, *_: (0,) * len(shape))
    scattered, terms = pl.pallas_call(
        field_kernel,
        grid_spec=pltpu.PrefetchScalarGridSpec(
            num_scalar_prefetch=3,
            grid=(classes,),
            in_specs=[
                whole(*cosine.shape),
                whole(*sine.shape),
                whole(2, dirs, modes),
                whole(2, all_spheres, modes),
                pl.BlockSpec((1, 2, modes, modes), lambda c, *_: (c, 0, 0, 0)),
            ],
            out_specs=[whole(2 * modes, spheres * dirs), whole(dirs, modes)],
            scratch_shapes=[
                pltpu.VMEM((cols, modes), jnp.float32),
                pltpu.VMEM((cols, modes), jnp.float32),
                pltpu.VMEM((blocks * cols, modes), jnp.bfloat16),
                pltpu.VMEM((blocks * cols, modes), jnp.bfloat16),
                pltpu.VMEM((blocks * cols, modes), jnp.bfloat16),
                pltpu.VMEM((blocks * cols, modes), jnp.float32),
                pltpu.VMEM((blocks * cols, modes), jnp.float32),
            ],
        ),
        out_shape=[
            jax.ShapeDtypeStruct((2 * modes, spheres * dirs), jnp.bfloat16),
            jax.ShapeDtypeStruct((dirs, modes), jnp.float32),
        ],
        compiler_params=pltpu.CompilerParams(
            dimension_semantics=("arbitrary",), vmem_limit_bytes=56 * 1024 * 1024
        ),
    )(
        starts,
        sources,
        jnp.full((1,), me, jnp.int32),
        cosine,
        sine,
        chosen,
        mie_rows,
        trans_table,
    )
    local_terms = jnp.broadcast_to(jnp.sum(terms, axis=1)[None], (devices, dirs))
    extinction = jnp.sum(
        lax.all_to_all(local_terms, "sph", split_axis=0, concat_axis=0, tiled=True), axis=0
    )
    return (scattered, extinction)


def solution(mesh):
    placed = (
        P("sph", None),
        P(),
        P(),
        P("groups"),
        P(None, None, "sph"),
        P(),
        P("sph", None),
        P("sph"),
        P("sph"),
        P("sph"),
    )
    return jax.shard_map(
        shards,
        mesh=mesh,
        in_specs=placed,
        out_specs=(P(None, ("groups", "sph")), P("groups")),
        check_vma=False,
    )
```
